256 devices in a mesh: panels: 256 (over z, x, y, core).
Axes of the slice: x: 4, y: 4, z: 8, core: 2. Of those that a mesh axis runs over, the one named last changes fastest.
Arguments:
- densities: bfloat16 [64, 524288], P(None, 'panels'), may hold values from -6 to 6
- cluster_basis: bfloat16 [64, 524288], P(None, 'panels'), may hold values from -0.125 to 0.125
- near_rows: int32 [49152], P('panels'), may hold values from 0 to 19, as said below
- near_blocks: bfloat16 [49152, 128, 128], P('panels'), may hold values from -0.15625 to 0.15625
- local_coef: bfloat16 [4096, 4, 64, 64], P('panels'), may hold values from -0.75 to 0.75
- level_coef: bfloat16 [256, 8, 64, 64], P('panels'), may hold values from -0.375 to 0.375
Outputs:
- adjoint_image: float32 [64, 524288], P(None, 'panels')
The draws below stay inside these ranges and needn't reach their ends.
Inputs may be any that keep to these rules, and one draw needn't show every extreme that they name: For near-field block p with q = p mod 192, near_rows[p] - q // 12 lies in 0 to 4: a block reads leaf blocks at most 2 away in Morton order.
All inputs are finite; a program needn't handle non-finite values.
Results may differ from the reference program's by a relative error of at most 0.0024.
Values may be sent and summed in bfloat16 or wider, within the bound.
A program may use at most 64 MiB of HBM per device.

```python
import jax
import jax.numpy as jnp
from jax import lax

R = 64
K = 64
BLK = 128
PAN_DEV = 2048
NEAR_COL = 12
HB = 2
DEVS = 256
PANELS = 524288
NBLK = 16
NEAR = 192
PAIRS = 49152
BLOCKS = 4096
LLOC = 4
GLEV = 8


def draw_near_rows(key, part):
    device_count = PAIRS // NEAR
    offsets = jax.random.randint(key, (device_count, NBLK, NEAR_COL), -HB, HB + 1).astype(jnp.int32)
    offsets = offsets.at[:, 0, 0].set(-HB)
    offsets = offsets.at[:, NBLK - 1, 0].set(HB)
    columns = jnp.arange(NBLK, dtype=jnp.int32)[None, :, None]
    return (columns + HB + offsets).reshape(PAIRS).astype(jnp.int32)


def block_levels(rng, dims, cuts, least, high):
    def one(axis_at, blocks):
        heights = jax.random.uniform(jax.random.fold_in(jax.random.fold_in(rng, 6), axis_at), (blocks,), jnp.float32, least / len(cuts), high / len(cuts))
        return jnp.repeat(jnp.exp(heights), dims[axis_at] // blocks).reshape((-1,) + (1,) * (len(dims) - axis_at - 1))

    factor_of = one(*cuts[0])
    for cut in cuts[1:]:
        factor_of = factor_of * one(*cut)
    return factor_of


def scatter_about(stream_key, extent, width, reach, shards=(), kind=jnp.bfloat16):
    values = jax.random.normal(stream_key, extent, jnp.float32) * width
    if len(shards) > 0:
        values = block_levels(stream_key, extent, shards, -0.22, 0.18) * values
    return jnp.clip(values, min=-reach, max=reach).astype(kind)


def setup_inputs(seed: int = 0) -> dict:
    arg_keys = jax.random.split(jax.random.key(seed), 7)
    densities = scatter_about(arg_keys[0], (R, PANELS), 1.0, 6.0, ((1, 256),))
    cluster_basis = scatter_about(arg_keys[1], (K, PANELS), PAN_DEV ** -0.5, 0.125, ((1, 256),))
    near_rows = draw_near_rows(jax.random.fold_in(arg_keys[6], 71), 0)
    near_blocks = scatter_about(arg_keys[3], (PAIRS, BLK, BLK), (BLK * NEAR_COL) ** -0.5, 0.15625, ((0, 256),))
    local_coef = scatter_about(arg_keys[4], (BLOCKS, LLOC, K, K), K ** -0.5, 0.75, ((0, 256),))
    level_coef = scatter_about(arg_keys[5], (DEVS, GLEV, K, K), (4 * K) ** -0.5, 0.375, ((0, 256),))
    return {"densities": densities, "cluster_basis": cluster_basis, "near_rows": near_rows, "near_blocks": near_blocks, "local_coef": local_coef, "level_coef": level_coef}


def reference(densities, cluster_basis, near_rows, near_blocks, local_coef, level_coef):
    f32 = jnp.float32
    highest = lax.Precision.HIGHEST
    dens_four = densities.reshape(R, DEVS, NBLK, BLK).astype(f32)
    basis_four = cluster_basis.reshape(K, DEVS, NBLK, BLK).astype(f32)
    block_summ = jnp.einsum('kdbp,rdbp->dbkr', basis_four, dens_four, precision=highest)
    device_sum = jnp.sum(block_summ, axis=1)
    level_list = []
    for level_no in range(GLEV):
        grouped = device_sum.reshape(DEVS >> level_no, 1 << level_no, K, R).sum(1)
        sibling = grouped.reshape(-1, 2, K, R)[:, ::-1].reshape(DEVS >> level_no, K, R)
        level_list.append(jnp.repeat(sibling, 1 << level_no, axis=0))
    level_in = jnp.stack(level_list, axis=1)
    global_part = jnp.einsum('dlkq,dlkr->dqr', level_coef.astype(f32), level_in, precision=highest)
    padded = jnp.pad(densities, ((0, 0), (HB * BLK, HB * BLK)))
    rows_all = near_rows.reshape(DEVS, NEAR)
    blocks_all = near_blocks.reshape(DEVS, NEAR, BLK, BLK)
    coef_all = local_coef.reshape(DEVS, NBLK, LLOC, K, K)
    basis_all = jnp.transpose(basis_four, (1, 0, 2, 3))
    device_ids = jnp.arange(DEVS, dtype=jnp.int32)

    def one_device(items):
        dev_no, summ, glob, basis_dev, rows_dev, blocks_dev, coef_dev = items
        local_part = jnp.zeros((NBLK, K, R), f32)
        for depth_no in range(LLOC):
            cluster_sums = summ.reshape(NBLK >> depth_no, 1 << depth_no, K, R).sum(1)
            sibling = cluster_sums.reshape(-1, 2, K, R)[:, ::-1].reshape(NBLK >> depth_no, K, R)
            partner = jnp.repeat(sibling, 1 << depth_no, axis=0)
            local_part = local_part + jnp.einsum('bkq,bkr->bqr', coef_dev[:, depth_no].astype(f32), partner, precision=highest)
        coupled = (local_part + glob[None]).astype(jnp.bfloat16)
        far = jnp.einsum('kbp,bkr->rbp', basis_dev, coupled.astype(f32), precision=highest)
        start = (dev_no * PAN_DEV).astype(jnp.int32)
        extended = lax.dynamic_slice_in_dim(padded, start, PAN_DEV + 2 * HB * BLK, axis=1)
        ext_blocks = extended.reshape(R, NBLK + 2 * HB, BLK)
        picked = jnp.take(ext_blocks, rows_dev.astype(jnp.int32), axis=1).astype(f32)
        terms = jnp.einsum('pij,rpi->rpj', blocks_dev.astype(f32), picked, precision=highest)
        near = terms.reshape(R, NBLK, NEAR_COL, BLK).sum(2)
        return (near + far).reshape(R, PAN_DEV)

    result = lax.map(one_device, (device_ids, block_summ, global_part, basis_all, rows_all, blocks_all, coef_all))
    return jnp.transpose(result, (1, 0, 2)).reshape(R, PANELS)
```

```python
import functools

import jax
import jax.numpy as jnp
from jax import lax
from jax.experimental import pallas as pl
from jax.experimental.pallas import tpu as pltpu
from jax.sharding import PartitionSpec as P

HB = 2
MESH = pl.DeviceIdType.MESH
F32 = jnp.float32
BF16 = jnp.bfloat16
STAGES = ((0, 3), (3, 2), (5, 3))


def flipped(me, mask):
    out = me
    bit = 1
    while bit <= mask:
        if mask & bit:
            out = out + bit * (1 - 2 * ((me // bit) % 2))
        bit *= 2
    return out


def nt(a, b):
    return lax.dot_general(a, b, (((1,), (1,)), ((), ())), preferred_element_type=F32)


def split(x):
    hi = x.astype(BF16)
    lo = (x - hi.astype(F32)).astype(BF16)
    return hi, lo


def kernel(
    devices,
    dens_h,
    basis_h,
    rows_h,
    near_h,
    local_h,
    level_h,
    out_h,
    dens,
    basis,
    rows,
    near,
    local,
    level,
    left,
    right,
    acc,
    twin,
    part,
    sums,
    slots,
    levels,
    in_sem,
    dens_sem,
    near_sem,
    send_sem,
    recv_sem,
    halo_send,
    halo_recv,
    out_sem,
):
    me = lax.axis_index("panels")
    width = dens.shape[1]
    rank = basis.shape[0]
    leaves, depth, blk = near.shape
    per = depth // blk
    edge = left.shape[0] - HB

    peers = []
    for low, bits in STAGES:
        peers.append([flipped(me, k << low) for k in range(1, 1 << bits)])
    after = lax.rem(me + 1, devices)
    before = lax.rem(me + devices - 1, devices)

    barrier = pltpu.get_barrier_semaphore()
    everyone = [p for group in peers for p in group] + [after, before]
    for p in everyone:
        pl.semaphore_signal(barrier, inc=1, device_id=(p,), device_id_type=MESH)

    loads = [
        pltpu.make_async_copy(basis_h, basis, in_sem.at[0]),
        pltpu.make_async_copy(rows_h, rows, in_sem.at[1]),
        pltpu.make_async_copy(local_h, local, in_sem.at[2]),
        pltpu.make_async_copy(level_h, level, in_sem.at[3]),
    ]

    def dens_load(b, target, sem):
        return pltpu.make_async_copy(dens_h.at[:, pl.ds(b * blk, blk)], target, sem)

    dens_loads = [dens_load(b, dens.at[b], dens_sem.at[b]) for b in range(leaves)]
    edge_loads = [
        dens_load(b, left.at[HB + b], dens_sem.at[leaves + b]) for b in range(edge)
    ] + [
        dens_load(leaves - edge + b, right.at[b], dens_sem.at[leaves + edge + b]) for b in range(edge)
    ]
    near_loads = [
        pltpu.make_async_copy(near_h.at[c], near.at[c], near_sem.at[c]) for c in range(leaves)
    ]
    for copy in dens_loads + loads + edge_loads:
        copy.start()
    order = list(range(HB, leaves - HB)) + [0, 1, leaves - 2, leaves - 1]
    for c in order:
        near_loads[c].start()

    lane = lax.broadcasted_iota(jnp.int32, (width, 2 * rank), 1) < rank
    half = width // 2
    lane_half = lax.broadcasted_iota(jnp.int32, (half, 2 * rank), 1) < rank

    for copy in dens_loads:
        copy.wait()
    loads[0].wait()
    u_all = basis[...]
    x_all = jnp.concatenate([dens[b] for b in range(leaves)], axis=1)
    both = nt(x_all, jnp.concatenate([u_all, u_all], axis=0))
    sums[0] = jnp.where(lane_half, both[:half], both[half:])

    def sends(stage):
        first = sum((1 << bits) - 1 for _, bits in STAGES[:stage])
        return [
            pltpu.make_async_remote_copy(
                src_ref=sums.at[stage],
                dst_ref=slots.at[first + i],
                send_sem=send_sem.at[first + i],
                recv_sem=recv_sem.at[first + i],
                device_id=(p,),
                device_id_type=MESH,
            )
            for i, p in enumerate(peers[stage])
        ]

    pl.semaphore_wait(barrier, len(everyone))
    stage_copies = [sends(s) for s in range(len(STAGES))]

    for copy in stage_copies[0]:
        copy.start()
    halo = [
        pltpu.make_async_remote_copy(
            src_ref=dens.at[pl.ds(leaves - HB, HB)],
            dst_ref=left.at[pl.ds(0, HB)],
            send_sem=halo_send.at[0],
            recv_sem=halo_recv.at[0],
            device_id=(after,),
            device_id_type=MESH,
        ),
        pltpu.make_async_remote_copy(
            src_ref=dens.at[pl.ds(0, HB)],
            dst_ref=right.at[pl.ds(edge, HB)],
            send_sem=halo_send.at[1],
            recv_sem=halo_recv.at[1],
            device_id=(before,),
            device_id_type=MESH,
        ),
    ]
    for copy in halo:
        copy.start()

    def collect(stage):
        low, bits = STAGES[stage]
        first = sum((1 << b) - 1 for _, b in STAGES[:stage])
        total = sums[stage]
        for l in range(bits):
            value = None
            for k in range(1 << l, 2 << l):
                stage_copies[stage][k - 1].wait_recv()
                slot = slots[first + k - 1]
                value = slot if value is None else value + slot
            levels[low + l] = value
            total = total + value
        if stage + 1 < len(STAGES):
            sums[stage + 1] = total
            for copy in stage_copies[stage + 1]:
                copy.start()

    def near_leaf(c, source, shift):
        near_loads[c].wait()
        picked = []
        for i in range(per):
            at = jnp.clip(rows[c * per + i] - shift, 0, source.shape[0] - 1)
            picked.append(source[at])
        acc[:, c * blk : (c + 1) * blk] = jnp.dot(
            jnp.concatenate(picked, axis=1), near[c], preferred_element_type=F32
        )

    def local_part():
        loads[2].wait()
        tree = []
        leaf_sums = []
        for b in range(leaves):
            u = basis[:, b * blk : (b + 1) * blk]
            leaf_sums.append(nt(dens[b], jnp.concatenate([u, u], axis=0)))
        tree.append(leaf_sums)
        while len(tree[-1]) > 2:
            last = tree[-1]
            tree.append([last[2 * i] + last[2 * i + 1] for i in range(len(last) // 2)])
        for b in range(leaves):
            sib = [tree[j][(b >> j) ^ 1] for j in range(4)]
            value = jnp.concatenate(
                [jnp.where(lane, sib[0], sib[1]), jnp.where(lane, sib[2], sib[3])], axis=1
            )
            hi, lo = split(value)
            weight = local[b].reshape(4 * rank, rank)
            twice = jnp.dot(jnp.concatenate([hi, lo], axis=0), weight, preferred_element_type=F32)
            part[b] = twice[:width] + twice[width:]

    def global_part(l0, l1):
        values = jnp.concatenate([levels[l] for l in range(l0, l1)], axis=1)
        hi, lo = split(values)
        stacked = jnp.concatenate([hi, lo], axis=0)
        zero = jnp.zeros((rank, rank), BF16)
        tops, bottoms = [], []
        for l in range(l0, l1):
            tops += [level[l], zero]
            bottoms += [zero, level[l]]
        top = jnp.dot(stacked, jnp.concatenate(tops, axis=0), preferred_element_type=F32)
        bottom = jnp.dot(stacked, jnp.concatenate(bottoms, axis=0), preferred_element_type=F32)
        return jnp.concatenate([top[:half] + top[half:], bottom[:half] + bottom[half:]], axis=0)

    local_part()
    collect(0)
    loads[1].wait()
    for c in range(HB, HB + 5):
        near_leaf(c, dens, HB)
    collect(1)
    for c in range(HB + 5, leaves - HB):
        near_leaf(c, dens, HB)
    for copy in edge_loads:
        copy.wait()
    for copy in halo:
        copy.wait_recv()

    @pl.when(me == 0)
    def _():
        left[:HB] = jnp.zeros((HB, width, blk), BF16)

    @pl.when(me == devices - 1)
    def _():
        right[edge:] = jnp.zeros((HB, width, blk), BF16)

    for c in range(HB):
        near_leaf(c, left, 0)
    for c in range(leaves - HB, leaves):
        near_leaf(c, right, leaves - HB)
    loads[3].wait()
    twin[...] = global_part(0, 5)
    collect(2)

    glob = twin[...] + global_part(5, 8)
    outs = []
    for b in range(leaves):
        coupled = (part[b] + glob).astype(BF16)
        cols = slice(b * blk, (b + 1) * blk)
        acc[:, cols] = acc[:, cols] + jnp.dot(coupled, basis[:, cols], preferred_element_type=F32)
        if b % 4 == 3:
            chunk = pl.ds((b - 3) * blk, 4 * blk)
            copy = pltpu.make_async_copy(acc.at[:, chunk], out_h.at[:, chunk], out_sem.at[b // 4])
            copy.start()
            outs.append(copy)

    for group in stage_copies:
        for copy in group:
            copy.wait_send()
    for copy in halo:
        copy.wait_send()
    for copy in outs:
        copy.wait()


def local_step(devices, densities, cluster_basis, near_rows, near_blocks, local_coef, level_coef):
    width, pans = densities.shape
    rank = cluster_basis.shape[0]
    pairs, blk, _ = near_blocks.shape
    leaves = pans // blk
    per = pairs // leaves
    near = near_blocks.reshape(leaves, per * blk, blk)
    level = level_coef[0]
    n_slots = sum((1 << bits) - 1 for _, bits in STAGES)
    n_levels = level.shape[0]
    edge = 2 * HB
    any_space = pl.BlockSpec(memory_space=pl.ANY)
    return pl.pallas_call(
        functools.partial(kernel, devices),
        out_shape=jax.ShapeDtypeStruct((width, pans), F32),
        in_specs=[any_space] * 6,
        out_specs=any_space,
        scratch_shapes=[
            pltpu.VMEM((leaves, width, blk), BF16),
            pltpu.VMEM((rank, pans), BF16),
            pltpu.SMEM((pairs,), jnp.int32),
            pltpu.VMEM(near.shape, BF16),
            pltpu.VMEM(local_coef.shape, BF16),
            pltpu.VMEM(level.shape, BF16),
            pltpu.VMEM((edge + HB, width, blk), BF16),
            pltpu.VMEM((edge + HB, width, blk), BF16),
            pltpu.VMEM((width, pans), F32),
            pltpu.VMEM((width, rank), F32),
            pltpu.VMEM((leaves, width, rank), F32),
            pltpu.VMEM((len(STAGES), width // 2, 2 * rank), F32),
            pltpu.VMEM((n_slots, width // 2, 2 * rank), F32),
            pltpu.VMEM((n_levels, width // 2, 2 * rank), F32),
            pltpu.SemaphoreType.DMA((4,)),
            pltpu.SemaphoreType.DMA((leaves + 2 * edge,)),
            pltpu.SemaphoreType.DMA((leaves,)),
            pltpu.SemaphoreType.DMA((n_slots,)),
            pltpu.SemaphoreType.DMA((n_slots,)),
            pltpu.SemaphoreType.DMA((2,)),
            pltpu.SemaphoreType.DMA((2,)),
            pltpu.SemaphoreType.DMA((4,)),
        ],
        compiler_params=pltpu.CompilerParams(
            collective_id=0, has_side_effects=True, vmem_limit_bytes=56 * 1024 * 1024
        ),
        name="adjoint",
    )(densities, cluster_basis, near_rows, near, local_coef, level)


def solution(mesh):
    devices = mesh.shape["panels"]
    return jax.shard_map(
        functools.partial(local_step, devices),
        mesh=mesh,
        in_specs=(
            P(None, "panels"),
            P(None, "panels"),
            P("panels"),
            P("panels", None, None),
            P("panels", None, None, None),
            P("panels", None, None, None),
        ),
        out_specs=P(None, "panels"),
        check_vma=False,
    )
```
